32 devices in a mesh: outer: 4 (over y, x), dev: 8 (over z, core).
Axes of the slice: x: 2, y: 2, z: 4, core: 2. Of those that a mesh axis runs over, the one named last changes fastest.
Arguments:
- documents: bfloat16 [6144, 4096], P(('outer', 'dev')), may hold values from -8 to 8
- cluster_of: int32 [6144], replicated, may hold values from 0 to 31, as said below
- neighbours: int32 [32, 4], replicated, may hold values from 0 to 31, as said below
- sharpness: float32 [32], replicated, may hold values from 32 to 64
Outputs:
- density: float32 [6144], P(('outer', 'dev'))
The draws below stay inside these ranges and needn't reach their ends.
Inputs may be any that keep to these rules, and one draw needn't show every extreme that they name: `cluster_of`: rows b * 192 to (b + 1) * 192 - 1 form block b. Block b names only clusters g * 8 to (g + 1) * 8 - 1, with g = b // 8, and names no cluster more than 48 times; in each group g some cluster is named exactly 48 times by every block of that group; every cluster is named by some row. `neighbours`: row c, with c = g * 8 + h, lists in order the clusters g * 8 + ((h - 1) mod 8), g * 8 + ((h + 1) mod 8), ((g - 1) mod 4) * 8 + ((h + b) mod 8) and ((g + 1) mod 4) * 8 + ((h + d) mod 8), with b and d each in -1, 0, 1.
All inputs are finite; a program needn't handle non-finite values.
Results may differ from the reference program's by a relative error of at most 0.00047.
Values may be sent and summed in bfloat16 or wider, within the bound.
A program may use at most 128 MiB of HBM per device.

```python
import math
import jax
import jax.numpy as jnp
from jax import lax

E = 4096
NEIGHBOURS = 4
TOK_DEV = 192
CLUSTER_GROUPS = 4
CLUSTERS_IN_GROUP = 8
CLUSTERS = 32
CAP = 48
SLOTS = 384
DOCS = 6144


theme_count = 32


def cluster_draw(key):
    blocks_total = CLUSTER_GROUPS * CLUSTERS_IN_GROUP
    tickets = CLUSTERS_IN_GROUP * CAP
    base_key = jax.random.fold_in(key, 7)
    split_points = jax.random.split(base_key, 4)
    extra_reward = jax.random.randint(split_points[0], (CLUSTER_GROUPS, CLUSTERS_IN_GROUP), 0, 4096)
    weighty_blocks = jax.random.randint(split_points[1], (CLUSTER_GROUPS,), 0, CLUSTERS_IN_GROUP)
    extra_reward = jnp.where(jnp.arange(CLUSTERS_IN_GROUP, dtype=jnp.int32)[None, :] == weighty_blocks[:, None], 32768, extra_reward)
    owner_of_ticket = jnp.arange(tickets, dtype=jnp.int32) // CAP
    ticket_copy = jnp.arange(tickets, dtype=jnp.int32) % CAP
    random_perturb = jax.random.randint(split_points[2], (blocks_total, tickets), 0, 4096)
    group_of_block = jnp.arange(blocks_total, dtype=jnp.int32) // CLUSTERS_IN_GROUP
    block_owner = jnp.arange(blocks_total, dtype=jnp.int32) % CLUSTERS_IN_GROUP
    compelled_choice = (owner_of_ticket[None, :] == block_owner[:, None]) & (ticket_copy[None, :] == 0)
    density_scores = random_perturb + extra_reward[group_of_block][:, owner_of_ticket] + jnp.where(compelled_choice, 65536, 0)
    density_scores = density_scores * tickets + jnp.arange(tickets, dtype=jnp.int32)[None, :]
    ranked, chosen = lax.top_k(density_scores, TOK_DEV)
    local_labels = owner_of_ticket[chosen]
    shuffled = jax.random.permutation(split_points[3], local_labels, axis=1, independent=True)
    labels_all = shuffled + group_of_block[:, None] * CLUSTERS_IN_GROUP
    return labels_all.reshape(-1).astype(jnp.int32)


def draw_cluster_of(key, part):
    return cluster_draw(key)


def draw_documents(key, part):
    labels_all = cluster_draw(key)
    base_key = jax.random.fold_in(key, 13)
    split_points = jax.random.split(base_key, 4)
    centres = jax.random.normal(split_points[0], (CLUSTERS, E), jnp.float32)
    themes = jax.random.normal(split_points[1], (theme_count, E), jnp.float32)
    picked = jax.random.randint(split_points[2], (DOCS,), 0, theme_count)
    noise = jax.random.normal(split_points[3], (DOCS, E), jnp.float32)
    theme_weight = 0.35
    values = centres[labels_all] + theme_weight * themes[picked] + noise
    return jnp.clip(values, -8.0, 8.0).astype(jnp.bfloat16)


def draw_neighbours(key, part):
    base_key = jax.random.fold_in(key, 17)
    offsets = jax.random.randint(base_key, (CLUSTERS, 2), -1, 2).astype(jnp.int32)
    cluster_range = jnp.arange(CLUSTERS, dtype=jnp.int32)
    group_of = cluster_range // CLUSTERS_IN_GROUP
    owner_of = cluster_range % CLUSTERS_IN_GROUP
    group_moves = jnp.stack([jnp.zeros_like(group_of), jnp.zeros_like(group_of), jnp.full_like(group_of, -1), jnp.ones_like(group_of)], axis=1)
    owner_moves = jnp.stack([jnp.full_like(owner_of, -1), jnp.ones_like(owner_of), offsets[:, 0], offsets[:, 1]], axis=1)
    group_next = (group_of[:, None] + group_moves + CLUSTER_GROUPS) % CLUSTER_GROUPS
    owner_next = (owner_of[:, None] + owner_moves + CLUSTERS_IN_GROUP) % CLUSTERS_IN_GROUP
    return (group_next * CLUSTERS_IN_GROUP + owner_next).astype(jnp.int32)


def setup_inputs(seed: int = 0) -> dict:
    key_of = jax.random.split(jax.random.key(seed), 5)
    return {
        "documents": draw_documents(jax.random.fold_in(key_of[4], 71), 0),
        "cluster_of": draw_cluster_of(jax.random.fold_in(key_of[4], 71), 0),
        "neighbours": draw_neighbours(jax.random.fold_in(key_of[4], 71), 0),
        "sharpness": jnp.clip(jnp.exp(jax.random.uniform(key_of[3], (CLUSTERS,), jnp.float32, math.log(32.0), math.log(64.0))), 32.0, 64.0),
    }


def reference(documents, cluster_of, neighbours, sharpness):
    count_blocks = DOCS // TOK_DEV
    cluster_sizes = jnp.zeros((CLUSTERS,), jnp.int32).at[cluster_of].add(1)
    cluster_sums = jax.ops.segment_sum(documents.astype(jnp.float32), cluster_of, num_segments=CLUSTERS)
    cluster_means = cluster_sums / cluster_sizes.astype(jnp.float32)[:, None]
    centred = documents.astype(jnp.float32) - cluster_means[cluster_of]
    scaling = lax.rsqrt(lax.optimization_barrier(jnp.mean(centred * centred, axis=1)) + 1e-06) / math.sqrt(E)
    unit_rows = (centred * scaling[:, None]).astype(jnp.bfloat16)
    block_labels = cluster_of.reshape(count_blocks, TOK_DEV)
    ordinal = jnp.arange(TOK_DEV, dtype=jnp.int32)
    earlier = ordinal[None, :] < ordinal[:, None]
    repeats = lax.optimization_barrier(jnp.sum(((block_labels[:, :, None] == block_labels[:, None, :]) & earlier[None]).astype(jnp.int32), axis=2))
    source_slot = (jnp.arange(count_blocks, dtype=jnp.int32) % CLUSTERS_IN_GROUP)[:, None]
    slot_of = (source_slot * CAP + repeats).reshape(-1).astype(jnp.int32)
    rows_index = jnp.arange(DOCS, dtype=jnp.int32)
    slot_table = jnp.zeros((CLUSTERS, SLOTS), jnp.int32).at[cluster_of, slot_of].set(rows_index)
    filled = jnp.zeros((CLUSTERS, SLOTS), jnp.float32).at[cluster_of, slot_of].set(1.0)
    off_diagonal = 1.0 - jnp.eye(SLOTS, dtype=jnp.float32)

    def per_cluster(cluster_index):
        queries = unit_rows[slot_table[cluster_index]]
        own_gain = sharpness[cluster_index]
        own_terms = jnp.exp(own_gain * jnp.dot(queries, queries.T, preferred_element_type=jnp.float32))
        running = lax.optimization_barrier(jnp.sum(own_terms * filled[cluster_index][None, :] * off_diagonal, axis=1))
        for position in range(NEIGHBOURS):
            partner = neighbours[cluster_index, position]
            key_rows = unit_rows[slot_table[partner]]
            pair_gain = 0.5 * (own_gain + sharpness[partner])
            kernel_terms = jnp.exp(pair_gain * jnp.dot(queries, key_rows.T, preferred_element_type=jnp.float32))
            running = running + lax.optimization_barrier(jnp.sum(kernel_terms * filled[partner][None, :], axis=1))
        partner_count = cluster_sizes[cluster_index] - 1 + jnp.sum(cluster_sizes[neighbours[cluster_index]])
        return jnp.log(running / partner_count.astype(jnp.float32))
    slot_density = lax.map(per_cluster, jnp.arange(CLUSTERS, dtype=jnp.int32))
    return slot_density[cluster_of, slot_of]
```

```python
import functools
import math

import jax
import jax.numpy as jnp
from jax import lax
from jax.experimental import pallas as pl
from jax.experimental.pallas import tpu as pltpu
from jax.sharding import PartitionSpec as P


def passed_along(block, axis, distance):
    devices = range(lax.axis_size(axis))
    route = [((i - distance) % len(devices), i) for i in devices]
    return lax.ppermute(block, axis, route)


def kernel_block(queries, others, pair_gain):
    products = jnp.einsum("qe,ke->qk", queries, others, preferred_element_type=jnp.float32)
    return jnp.exp(pair_gain * products)


def shards(documents, cluster_of, neighbours, sharpness):
    groups = lax.axis_size("outer")
    owners = lax.axis_size("dev")
    tokens_here = documents.shape[0]
    feature_width = documents.shape[1]
    capacity = max(2, 2 * tokens_here // owners)
    slot_count = owners * capacity
    group_index = lax.axis_index("outer")
    owner_index = lax.axis_index("dev")
    own_cluster = group_index * owners + owner_index
    block_labels = cluster_of.reshape(groups * owners, tokens_here)
    group_of_block = jnp.arange(groups * owners, dtype=jnp.int32) // owners
    local_labels = block_labels - group_of_block[:, None] * owners
    owner_range = jnp.arange(owners, dtype=jnp.int32)
    per_block = jnp.sum(
        (local_labels[:, :, None] == owner_range).astype(jnp.int32), axis=1
    ).reshape(groups, owners, owners)
    cluster_sizes = jnp.sum(per_block, axis=1).reshape(-1)
    own_labels = lax.dynamic_index_in_dim(local_labels, own_cluster, 0, keepdims=False)
    ordinal = jnp.arange(tokens_here, dtype=jnp.int32)
    earlier = ordinal[None, :] < ordinal[:, None]
    repeats = jnp.sum(
        ((own_labels[:, None] == own_labels[None, :]) & earlier).astype(jnp.int32), axis=1
    )
    target = own_labels * capacity + repeats
    placing = (jnp.arange(slot_count, dtype=jnp.int32)[:, None] == target[None, :]).astype(
        jnp.bfloat16
    )
    outgoing = jnp.dot(placing, documents, preferred_element_type=jnp.float32).astype(jnp.bfloat16)
    arrived = lax.all_to_all(
        outgoing.reshape(owners, capacity, feature_width),
        "dev",
        split_axis=0,
        concat_axis=0,
        tiled=True,
    ).reshape(slot_count, feature_width)

    def slot_mask(group_at, owner_at):
        senders = per_block[group_at, :, owner_at]
        return (
            (jnp.arange(capacity, dtype=jnp.int32)[None, :] < senders[:, None])
            .astype(jnp.float32)
            .reshape(-1)
        )

    present = slot_mask(group_index, owner_index)
    centre = jnp.dot(
        present.astype(jnp.bfloat16)[None, :], arrived, preferred_element_type=jnp.float32
    )[0]
    centre = centre / cluster_sizes[own_cluster].astype(jnp.float32)
    centred = arrived.astype(jnp.float32) - centre[None, :]
    scaling = lax.rsqrt(jnp.mean(centred * centred, axis=1) + 1e-06) / math.sqrt(feature_width)
    unit_rows = (centred * (scaling * present)[:, None]).astype(jnp.bfloat16)
    own_gain = sharpness[own_cluster]
    listed = neighbours[own_cluster]
    off_diagonal = 1.0 - jnp.eye(slot_count, dtype=jnp.float32)
    running = jnp.sum(
        kernel_block(unit_rows, unit_rows, own_gain) * (present[None, :] * off_diagonal), axis=1
    )
    beside = [passed_along(unit_rows, "dev", offset) for offset in (1, -1)]
    vertical = []
    for direction, position in ((1, 2), (-1, 3)):
        receiver_group = (group_index + direction) % groups
        wanted = neighbours[receiver_group * owners + owner_index, position]
        delta = (wanted % owners - owner_index + owners) % owners
        picked_rows = jnp.where(
            delta == 1, beside[1], jnp.where(delta == owners - 1, beside[0], unit_rows)
        )
        vertical.append(passed_along(picked_rows, "outer", direction))
    key_sets = [beside[0], beside[1], vertical[0], vertical[1]]
    for position in range(4):
        partner = listed[position]
        partner_group_at = partner // owners
        partner_owner_at = partner % owners
        partner_partner = partner_group_at * owners + partner_owner_at
        pair_gain = 0.5 * (own_gain + sharpness[partner_partner])
        partner = partner_partner
        kernel_terms = kernel_block(unit_rows, key_sets[position], pair_gain)
        key_mask = slot_mask(partner_group_at, partner_owner_at)
        running = running + jnp.sum(kernel_terms * key_mask[None, :], axis=1)
    partner_count = cluster_sizes[own_cluster] - 1 + jnp.sum(cluster_sizes[listed])
    slot_density = jnp.log(running / partner_count.astype(jnp.float32))
    answered = lax.all_to_all(
        slot_density.reshape(owners, capacity), "dev", split_axis=0, concat_axis=0, tiled=True
    ).reshape(-1)
    return answered[target]


MESH = pl.DeviceIdType.MESH


PIECES = 16
GROUPED = 4


def start(copy):
    copy.start()


def sent(copy):
    copy.wait_send()


def landed(copy):
    copy.wait_recv()


def loop(count, body):
    lax.fori_loop(0, count, lambda k, carry: (body(k), carry)[1], 0)


def density_kernel(
    docs_ref, cluster_ref, neighbours_ref, sharpness_ref, out_ref,
    keys, queries, part, pair_half, chip_half, line_in, line_half, middle_in, sums, triple,
    centred, squares, labels_ref, lists_ref, gain_ref, klist_ref, kgain_ref, kscale_ref,
    alpha, products, acc_ref, cols_ref, returned_ref, rows_ref, rows_in,
    load_sems, stage_sems, z_sems, core_sems, key_sems, side_sems, relay_sems, flow_sems,
    scale_sems, return_sems, row_sems,
):
    dev = lax.axis_index("dev")
    group = lax.axis_index("outer")
    z, core = dev // 2, lax.rem(dev, 2)
    odd = lax.rem(group, 2)
    rows, width = docs_ref.shape
    span = width // PIECES
    half = PIECES // 2
    clusters = neighbours_ref.shape[1]
    base = group * 8
    partner_at = 2 * z + 1 - core
    partner = {"dev": partner_at}
    above = {"dev": lax.rem(dev + 2, 8)}
    below = {"dev": lax.rem(dev + 6, 8)}
    beside_group = group + 1 - 2 * odd
    opposite_group = 3 - group
    beside = {"outer": beside_group}
    opposite = {"outer": opposite_group}
    across = {"outer": lax.rem(group + 2, 4)}
    others = [lax.rem(dev + step, 8) for step in range(1, 8)]

    def loading(k):
        return pltpu.make_async_copy(
            docs_ref.at[:, pl.ds(pl.multiple_of(k * span, span), span)],
            keys.at[dev, k],
            load_sems.at[k],
        )

    loop(PIECES, lambda k: loading(k).start())
    barrier = pltpu.get_barrier_semaphore()
    peers = [{"dev": peer} for peer in others] + [beside, opposite, across]
    for peer in peers:
        pl.semaphore_signal(barrier, inc=1, device_id=peer, device_id_type=MESH)

    square = (rows, rows)
    same = lax.broadcasted_iota(jnp.int32, square, 0) == lax.broadcasted_iota(jnp.int32, square, 1)
    lane = lax.broadcasted_iota(jnp.int32, (1, 128), 1)

    def fetch_labels(slot, block):
        top = 3 * (block // 2)
        late = lax.rem(block, 2)
        first = cluster_ref[pl.ds(top, 1), :]
        middle = cluster_ref[pl.ds(top + 1, 1), :]
        last = cluster_ref[pl.ds(top + 2, 1), :]
        turned = jnp.where(lane < 64, pltpu.roll(middle, 64, 1), pltpu.roll(last, 64, 1))
        tail = jnp.where(late == 1, pltpu.roll(last, 64, 1), middle)
        labels_ref[slot, :, 0:128] = jnp.where(late == 1, turned, first)
        labels_ref[slot, :, 128:rows] = tail[:, 0 : rows - 128]

    loop(8, lambda at: fetch_labels(at, base + at))
    fetch_labels(8, beside_group * 8 + dev)
    fetch_labels(9, opposite_group * 8 + dev)
    own_labels = labels_ref[dev]
    member = (
        own_labels == base + lax.broadcasted_iota(jnp.int32, (8, rows), 0)
    ).astype(jnp.bfloat16)

    def partial_sums(k):
        loading(k).wait()
        part[k] = jnp.dot(member, keys[dev, k], preferred_element_type=jnp.float32)

    loop(PIECES, partial_sums)
    pl.semaphore_wait(barrier, len(peers))

    def remote(src, dst, send_sem, recv_sem, device):
        return pltpu.make_async_remote_copy(
            src_ref=src, dst_ref=dst, send_sem=send_sem, recv_sem=recv_sem,
            device_id=device, device_id_type=MESH,
        )

    def hop(unit, k, device):
        at = 2 * unit + core
        return remote(
            keys.at[at, k], keys.at[at, k], z_sems.at[unit], key_sems.at[at, k], device
        )

    def share(unit, k):
        at = 2 * unit + core
        return remote(
            keys.at[at, k], keys.at[at, k], core_sems.at[unit], key_sems.at[at, k], partner
        )

    def whole_sent(unit, sems):
        at = 2 * unit + core
        remote(keys.at[at], keys.at[at], sems.at[unit], key_sems.at[at, 0], partner).wait_send()

    def arrived(at, k):
        remote(
            keys.at[at, k], keys.at[at, k], core_sems.at[0], key_sems.at[at, k], partner
        ).wait_recv()

    def side(k):
        return remote(
            queries.at[k, 0], queries.at[k, 1], flow_sems.at[0], side_sems.at[k], beside
        )

    def relay(k):
        return remote(
            queries.at[k, 1], queries.at[k, 2], flow_sems.at[1], relay_sems.at[k], across
        )

    mine = pl.ds(pl.multiple_of(core * half, half), half)
    theirs = pl.ds(pl.multiple_of((1 - core) * half, half), half)

    def staged(n, src, dst, device):
        return remote(src, dst, stage_sems.at[n, 0], stage_sems.at[n, 1], device)

    pairing = staged(0, part.at[theirs], pair_half, partner)
    lower = staged(1, chip_half, line_in, above)
    upper = staged(1, chip_half, line_in, below)
    rising = staged(2, line_half, middle_in, above)
    sinking = staged(2, line_half, middle_in, below)
    outward_up = staged(3, sums.at[mine], sums.at[mine], above)
    outward_down = staged(3, sums.at[mine], sums.at[mine], below)
    joining = staged(4, sums.at[mine], sums.at[mine], partner)

    def own_hops(first, stop):
        def one(k):
            @pl.when(z < 2)
            def _():
                hop(z, k, above).start()

            @pl.when(z == 3)
            def _():
                hop(z, k, below).start()

        lax.fori_loop(first, stop, lambda k, carry: (one(k), carry)[1], 0)

    pairing.start()
    own_hops(0, 1)

    @pl.when(z == 1)
    def _():
        own_hops(1, 3)

    loop(PIECES, lambda k: share(z, k).start())
    pairing.wait_recv()
    chip_half[...] = part[mine] + pair_half[...]

    @pl.when(z == 0)
    def _():
        lower.start()

    @pl.when(z == 3)
    def _():
        upper.start()

    @pl.when((z == 0) | (z == 3))
    def _():
        own_hops(1, PIECES)

    @pl.when((z == 1) | (z == 2))
    def _():
        lower.wait_recv()
        line_half[...] = chip_half[...] + line_in[...]

        @pl.when(z == 1)
        def _():
            rising.start()
            own_hops(3, PIECES)

        @pl.when(z == 2)
        def _():
            sinking.start()

        rising.wait_recv()
        sums[mine] = line_half[...] + middle_in[...]

        @pl.when(z == 1)
        def _():
            outward_down.start()

        @pl.when(z == 2)
        def _():
            outward_up.start()

    @pl.when((z == 0) | (z == 3))
    def _():
        outward_up.wait_recv()

    joining.start()

    def chosen(read, labels, first, zero):
        found = jnp.full(labels.shape, zero, jnp.float32)
        for h in range(8):
            found = jnp.where(labels == first + h, read(first + h), found)
        return found

    def listed(position):
        return lambda c: neighbours_ref[position, c].astype(jnp.float32)

    def sharp(c):
        return sharpness_ref[c]

    def upright(row):
        return jnp.sum(jnp.where(same, row, 0.0), axis=1, keepdims=True)

    def flat(column):
        return jnp.sum(jnp.where(same, column, 0.0), axis=0, keepdims=True)

    def count_of(c):
        hits = jnp.where(cluster_ref[...] == c, 1.0, 0.0)
        return jnp.sum(jnp.sum(hits, axis=0, keepdims=True), axis=1, keepdims=True)

    own_row = own_labels.astype(jnp.float32)
    own_upright = upright(own_row)
    lists_ref[0, 0] = own_upright
    upright_member = (
        own_upright
        == base.astype(jnp.float32)
        + lax.rem(lax.broadcasted_iota(jnp.int32, (rows, 24), 1), 8).astype(jnp.float32)
    ).astype(jnp.bfloat16)
    local = lax.broadcasted_iota(jnp.int32, (8, 1), 0)
    own_sizes = jnp.zeros((8, 1), jnp.float32)
    for h in range(8):
        own_sizes = jnp.where(local == h, count_of(base + h), own_sizes)

    joining.wait_recv()
    squares[...] = jnp.zeros_like(squares)

    def centre_piece(k):
        means = sums[k] / own_sizes
        high = means.astype(jnp.bfloat16).astype(jnp.float32)
        rest = means - high
        mid = rest.astype(jnp.bfloat16).astype(jnp.float32)
        parts = jnp.concatenate([high, mid, rest - mid], axis=0).astype(jnp.bfloat16)
        triple[k] = parts
        centre = jnp.dot(upright_member, parts, preferred_element_type=jnp.float32)
        moved = keys[dev, k].astype(jnp.float32) - centre
        centred[k] = moved
        squares[...] += moved * moved

    loop(PIECES, centre_piece)
    energy = jnp.sum(squares[...], axis=1, keepdims=True) / width
    scaling = lax.rsqrt(energy + 1e-06) / math.sqrt(width)

    def unit_piece(k):
        queries[k, 0] = (centred[k] * scaling).astype(jnp.bfloat16)

        @pl.when(k > 0)
        def _():
            side(k - 1).start()

    loop(PIECES, unit_piece)
    kscale_ref[dev] = flat(scaling)
    side(PIECES - 1).start()

    def scale_out(n):
        return remote(
            kscale_ref.at[dev], kscale_ref.at[dev],
            scale_sems.at[0, n], scale_sems.at[1, dev], {"dev": others[n]},
        )

    for n in range(7):
        scale_out(n).start()

    def onward(k):
        @pl.when(z == 1)
        def _():
            arrived(core, k)
            hop(0, k, above).start()
            share(0, k).start()

        @pl.when(z == 2)
        def _():
            arrived(6 + core, k)
            hop(3, k, below).start()
            share(3, k).start()
            arrived(2 + core, k)
            share(1, k).start()

    loop(half, onward)

    for b, slot in ((0, dev), (1, 8), (2, 9)):
        first = (base, beside_group * 8, opposite_group * 8)[b]
        labels = labels_ref[slot]
        if b > 0:
            lists_ref[b, 0] = upright(labels.astype(jnp.float32))
        gain_ref[b] = upright(chosen(sharp, labels, first, 0.0))
        positions = ((0, 1), (2 + odd,), (3 - odd,))[b]
        for place, position in enumerate(positions):
            lists_ref[b, 1 + place] = upright(chosen(listed(position), labels, first, 0.0))

    def key_tables(at):
        labels = labels_ref[at]
        klist_ref[at, 0] = labels.astype(jnp.float32)
        kgain_ref[at] = chosen(sharp, labels, base, 0.0)
        klist_ref[at, 1] = chosen(listed(3 - odd), labels, base, 0.0)
        klist_ref[at, 2] = chosen(listed(2 + odd), labels, base, 0.0)

    loop(8, key_tables)
    acc_ref[...] = jnp.zeros_like(acc_ref)
    own_lists = [chosen(listed(position), own_labels, base, 0.0) for position in range(4)]

    def add_count(c, total):
        here = c.astype(jnp.float32)
        found = jnp.where(own_row == here, 1.0, 0.0)
        for row in own_lists:
            found = found + jnp.where(row == here, 1.0, 0.0)
        return total + found * count_of(c)

    partner_count = lax.fori_loop(0, clusters, add_count, jnp.full((1, rows), -1.0, jnp.float32))

    def steps(k):
        side(k).wait_recv()
        relay(k).start()

        @pl.when(k < half)
        def _():
            onward(k + half)

        @pl.when((z == 1) & (k > 1))
        def _():
            arrived(6 + core, k - 2)
            hop(3, k - 2, below).start()
            share(3, k - 2).start()

    loop(PIECES, steps)

    @pl.when(z == 1)
    def _():
        for k in (PIECES - 2, PIECES - 1):
            arrived(6 + core, k)
            hop(3, k, below).start()
            share(3, k).start()

    def late(k):
        relay(k).wait_recv()

        @pl.when(z == 0)
        def _():
            arrived(6 + core, k)
            share(3, k).start()

    loop(PIECES, late)
    contract = (((1,), (1,)), ((), ()))

    def stacked(k):
        return queries[k].reshape(3 * rows, span)

    alpha[...] = jnp.zeros_like(alpha)

    def project(k):
        alpha[...] += lax.dot_general(
            stacked(k), triple[k], contract, preferred_element_type=jnp.float32
        )

    loop(PIECES, project)

    def multiplied(at, k):
        return lax.dot_general(
            stacked(k), keys[at, k], contract, preferred_element_type=jnp.float32
        )

    cluster_24 = base + lax.rem(lax.broadcasted_iota(jnp.int32, (24, rows), 0), 8)

    def finish(at, slot):
        @pl.when(at != dev)
        def _():
            remote(
                kscale_ref.at[at], kscale_ref.at[at],
                scale_sems.at[0, 0], scale_sems.at[1, at], partner,
            ).wait_recv()

        hot = jnp.where(labels_ref[at] == cluster_24, 1.0, 0.0)
        down = jnp.zeros((1, rows), jnp.float32)
        kl = klist_ref[at, 0]
        scale = 0.5 * kscale_ref[at]
        for b in range(3):
            strip = pl.ds(b * rows, rows)
            shift = jnp.dot(
                alpha[strip, :], hot,
                precision=lax.Precision.HIGHEST,
                preferred_element_type=jnp.float32,
            )
            terms = jnp.exp(
                (gain_ref[b] + kgain_ref[at]) * (scale * (products[slot, strip, :] - shift))
            )
            wanted = lists_ref[b, 1] == kl
            if b == 0:
                wanted = wanted | (lists_ref[0, 2] == kl) | (lists_ref[0, 0] == kl)
                wanted = wanted & jnp.logical_not(same & (at == dev))
                back = wanted
            else:
                back = lists_ref[b, 0] == klist_ref[at, b]
            acc_ref[b] += jnp.where(wanted, terms, 0.0)
            down = down + jnp.sum(jnp.where(back, terms, 0.0), axis=0, keepdims=True)
        cols_ref[at] = down

    def give_back(at):
        return remote(
            cols_ref.at[at], returned_ref.at[dev],
            return_sems.at[0, at], return_sems.at[1, dev], {"dev": at},
        )

    def whole_block(at):
        @pl.when(at != dev)
        def _():
            @pl.when(lax.rem(at, 2) != core)
            def _():
                loop(PIECES, lambda k: arrived(at, k))

        def gather(n):
            found = multiplied(at, n * GROUPED)
            for k in range(1, GROUPED):
                found = found + multiplied(at, n * GROUPED + k)
            return found

        products[0] = gather(0)

        def more(n, carry):
            products[0] += gather(n)
            return carry

        lax.fori_loop(1, PIECES // GROUPED, more, 0)
        finish(at, 0)

    def stage(n):
        unit = jnp.where(n == 0, z, jnp.where((n == 1) & (z == 1), 0, jnp.where((n == 1) & (z == 2), 1, 3)))
        ready = (n == 0) | ((n == 1) & (z < 3)) | ((n == 2) & ((z == 1) | (z == 2)))

        @pl.when(ready)
        def _():
            loop(2, lambda c: whole_block(2 * unit + c))

            @pl.when(n > 0)
            def _():
                loop(2, lambda c: give_back(2 * unit + c).start())

    loop(3, stage)

    @pl.when(z == 2)
    def _():
        products[...] = jnp.zeros_like(products)

        def stream(k):
            @pl.when(k < PIECES)
            def _():
                arrived(core, k)
                share(0, k).start()

            @pl.when(k > 0)
            def _():
                products[0] += multiplied(core, k - 1)
                arrived(1 - core, k - 1)
                products[1] += multiplied(1 - core, k - 1)

        loop(PIECES + 1, stream)
        finish(core, 0)
        finish(1 - core, 1)
        loop(2, lambda c: give_back(c).start())

    for b in range(3):
        rows_ref[b] = flat(jnp.sum(acc_ref[b], axis=1, keepdims=True))

    def row_back(b, device):
        return remote(
            rows_ref.at[b], rows_in.at[b - 1], row_sems.at[0, b - 1], row_sems.at[1, b - 1], device
        )

    row_back(1, beside).start()
    row_back(2, opposite).start()

    def came_back(sender):
        remote(
            cols_ref.at[0], returned_ref.at[sender],
            return_sems.at[0, 0], return_sems.at[1, sender], partner,
        ).wait_recv()

    cols_ref[dev] = rows_ref[0]

    def collect(sender):
        unit = sender // 2
        gives = (
            ((z == 0) & ((unit == 1) | (unit == 2)))
            | ((z == 1) & (unit == 2))
            | ((z == 3) & (unit < 3))
        )

        @pl.when(gives)
        def _():
            came_back(sender)
            cols_ref[dev] += returned_ref[sender]

    loop(8, collect)
    row_back(1, beside).wait_recv()
    row_back(2, opposite).wait_recv()
    total = cols_ref[dev] + rows_in[0] + rows_in[1]
    out_ref[...] = jnp.log(total / partner_count)

    pairing.wait_send()
    joining.wait_send()
    whole_sent(z, core_sems)
    remote(queries.at[:, 0], queries.at[:, 1], flow_sems.at[0], side_sems.at[0], beside).wait_send()
    remote(queries.at[:, 1], queries.at[:, 2], flow_sems.at[1], relay_sems.at[0], across).wait_send()
    row_back(1, beside).wait_send()
    row_back(2, opposite).wait_send()
    for n in range(7):
        scale_out(n).wait_send()

    def scale_rest(at):
        unit = at // 2
        used = (
            (unit == z)
            | ((z == 0) & (unit == 3))
            | ((z == 1) & ((unit == 0) | (unit == 3)))
            | ((z == 2) & ((unit == 0) | (unit == 1) | (unit == 3)))
        )

        @pl.when(jnp.logical_not(used))
        def _():
            remote(
                kscale_ref.at[at], kscale_ref.at[at],
                scale_sems.at[0, 0], scale_sems.at[1, at], partner,
            ).wait_recv()

    loop(8, scale_rest)

    def returns_sent(unit):
        loop(2, lambda c: give_back(2 * unit + c).wait_send())

    @pl.when(z != 2)
    def _():
        whole_sent(z, z_sems)

    @pl.when((z == 0) | (z == 3))
    def _():
        lower.wait_send()

    @pl.when((z == 1) | (z == 2))
    def _():
        rising.wait_send()
        outward_up.wait_send()

    @pl.when(z == 0)
    def _():
        whole_sent(3, core_sems)
        returns_sent(3)

    @pl.when(z == 1)
    def _():
        whole_sent(0, z_sems)
        whole_sent(3, z_sems)
        whole_sent(0, core_sems)
        whole_sent(3, core_sems)
        returns_sent(0)
        returns_sent(3)

    @pl.when(z == 2)
    def _():
        whole_sent(3, z_sems)
        for unit in (0, 1, 3):
            whole_sent(unit, core_sems)
            returns_sent(unit)


def gathered(documents, cluster_of, neighbours, sharpness):
    rows, width = documents.shape
    span = width // PIECES
    half = PIECES // 2
    vmem = pl.BlockSpec(memory_space=pltpu.VMEM)
    smem = pl.BlockSpec(memory_space=pltpu.SMEM)
    f32 = functools.partial(pltpu.VMEM, dtype=jnp.float32)
    bf16 = functools.partial(pltpu.VMEM, dtype=jnp.bfloat16)
    sems = pltpu.SemaphoreType.DMA
    density = pl.pallas_call(
        density_kernel,
        out_shape=jax.ShapeDtypeStruct((1, rows), jnp.float32),
        in_specs=[pl.BlockSpec(memory_space=pl.ANY), vmem, smem, smem],
        out_specs=vmem,
        scratch_shapes=[
            bf16((8, PIECES, rows, span)),
            bf16((PIECES, 3, rows, span)),
            f32((PIECES, 8, span)),
            f32((half, 8, span)),
            f32((half, 8, span)),
            f32((half, 8, span)),
            f32((half, 8, span)),
            f32((half, 8, span)),
            f32((PIECES, 8, span)),
            bf16((PIECES, 24, span)),
            f32((PIECES, rows, span)),
            f32((rows, span)),
            pltpu.VMEM((10, 1, rows), jnp.int32),
            f32((3, 3, rows, 1)),
            f32((3, rows, 1)),
            f32((8, 3, 1, rows)),
            f32((8, 1, rows)),
            f32((8, 1, rows)),
            f32((3 * rows, 24)),
            f32((2, 3 * rows, rows)),
            f32((3, rows, rows)),
            f32((8, 1, rows)),
            f32((8, 1, rows)),
            f32((3, 1, rows)),
            f32((2, 1, rows)),
            sems((PIECES,)),
            sems((5, 2)),
            sems((4,)),
            sems((4,)),
            sems((8, PIECES)),
            sems((PIECES,)),
            sems((PIECES,)),
            sems((2,)),
            sems((2, 8)),
            sems((2, 8)),
            sems((2, 2)),
        ],
        compiler_params=pltpu.CompilerParams(
            collective_id=0, has_side_effects=True, vmem_limit_bytes=56 * 1024 * 1024
        ),
        name="density",
    )(documents, cluster_of.reshape(-1, 128), neighbours.T, sharpness)
    return density.reshape(rows)


def solution(mesh):
    small = mesh.shape["dev"] == 8 and mesh.shape["outer"] == 4
    in_specs = (P(("outer", "dev"), None), P(), P(), P())
    out_specs = P(("outer", "dev"))
    body = gathered if small else shards
    return jax.shard_map(body, mesh=mesh, in_specs=in_specs, out_specs=out_specs, check_vma=False)
```

```python
import functools
import math

import jax
import jax.numpy as jnp
from jax import lax
from jax.experimental import pallas as pl
from jax.experimental.pallas import tpu as pltpu
from jax.sharding import PartitionSpec as P


def passed_along(block, axis, distance):
    devices = range(lax.axis_size(axis))
    route = [((i - distance) % len(devices), i) for i in devices]
    return lax.ppermute(block, axis, route)


def kernel_block(queries, others, pair_gain):
    products = jnp.einsum("qe,ke->qk", queries, others, preferred_element_type=jnp.float32)
    return jnp.exp(pair_gain * products)


def shards(documents, cluster_of, neighbours, sharpness):
    groups = lax.axis_size("outer")
    owners = lax.axis_size("dev")
    tokens_here = documents.shape[0]
    feature_width = documents.shape[1]
    capacity = max(2, 2 * tokens_here // owners)
    slot_count = owners * capacity
    group_index = lax.axis_index("outer")
    owner_index = lax.axis_index("dev")
    own_cluster = group_index * owners + owner_index
    block_labels = cluster_of.reshape(groups * owners, tokens_here)
    group_of_block = jnp.arange(groups * owners, dtype=jnp.int32) // owners
    local_labels = block_labels - group_of_block[:, None] * owners
    owner_range = jnp.arange(owners, dtype=jnp.int32)
    per_block = jnp.sum(
        (local_labels[:, :, None] == owner_range).astype(jnp.int32), axis=1
    ).reshape(groups, owners, owners)
    cluster_sizes = jnp.sum(per_block, axis=1).reshape(-1)
    own_labels = lax.dynamic_index_in_dim(local_labels, own_cluster, 0, keepdims=False)
    ordinal = jnp.arange(tokens_here, dtype=jnp.int32)
    earlier = ordinal[None, :] < ordinal[:, None]
    repeats = jnp.sum(
        ((own_labels[:, None] == own_labels[None, :]) & earlier).astype(jnp.int32), axis=1
    )
    target = own_labels * capacity + repeats
    placing = (jnp.arange(slot_count, dtype=jnp.int32)[:, None] == target[None, :]).astype(
        jnp.bfloat16
    )
    outgoing = jnp.dot(placing, documents, preferred_element_type=jnp.float32).astype(jnp.bfloat16)
    arrived = lax.all_to_all(
        outgoing.reshape(owners, capacity, feature_width),
        "dev",
        split_axis=0,
        concat_axis=0,
        tiled=True,
    ).reshape(slot_count, feature_width)

    def slot_mask(group_at, owner_at):
        senders = per_block[group_at, :, owner_at]
        return (
            (jnp.arange(capacity, dtype=jnp.int32)[None, :] < senders[:, None])
            .astype(jnp.float32)
            .reshape(-1)
        )

    present = slot_mask(group_index, owner_index)
    centre = jnp.dot(
        present.astype(jnp.bfloat16)[None, :], arrived, preferred_element_type=jnp.float32
    )[0]
    centre = centre / cluster_sizes[own_cluster].astype(jnp.float32)
    centred = arrived.astype(jnp.float32) - centre[None, :]
    scaling = lax.rsqrt(jnp.mean(centred * centred, axis=1) + 1e-06) / math.sqrt(feature_width)
    unit_rows = (centred * (scaling * present)[:, None]).astype(jnp.bfloat16)
    own_gain = sharpness[own_cluster]
    listed = neighbours[own_cluster]
    off_diagonal = 1.0 - jnp.eye(slot_count, dtype=jnp.float32)
    running = jnp.sum(
        kernel_block(unit_rows, unit_rows, own_gain) * (present[None, :] * off_diagonal), axis=1
    )
    beside = [passed_along(unit_rows, "dev", offset) for offset in (1, -1)]
    vertical = []
    for direction, position in ((1, 2), (-1, 3)):
        receiver_group = (group_index + direction) % groups
        wanted = neighbours[receiver_group * owners + owner_index, position]
        delta = (wanted % owners - owner_index + owners) % owners
        picked_rows = jnp.where(
            delta == 1, beside[1], jnp.where(delta == owners - 1, beside[0], unit_rows)
        )
        vertical.append(passed_along(picked_rows, "outer", direction))
    key_sets = [beside[0], beside[1], vertical[0], vertical[1]]
    for position in range(4):
        partner = listed[position]
        partner_group_at = partner // owners
        partner_owner_at = partner % owners
        partner_partner = partner_group_at * owners + partner_owner_at
        pair_gain = 0.5 * (own_gain + sharpness[partner_partner])
        partner = partner_partner
        kernel_terms = kernel_block(unit_rows, key_sets[position], pair_gain)
        key_mask = slot_mask(partner_group_at, partner_owner_at)
        running = running + jnp.sum(kernel_terms * key_mask[None, :], axis=1)
    partner_count = cluster_sizes[own_cluster] - 1 + jnp.sum(cluster_sizes[listed])
    slot_density = jnp.log(running / partner_count.astype(jnp.float32))
    answered = lax.all_to_all(
        slot_density.reshape(owners, capacity), "dev", split_axis=0, concat_axis=0, tiled=True
    ).reshape(-1)
    return answered[target]


MESH = pl.DeviceIdType.MESH


PIECES = 16
GROUPED = 4


def start(copy):
    copy.start()


def sent(copy):
    copy.wait_send()


def landed(copy):
    copy.wait_recv()


def loop(count, body):
    lax.fori_loop(0, count, lambda k, carry: (body(k), carry)[1], 0)


def density_kernel(
    docs_ref, cluster_ref, neighbours_ref, sharpness_ref, out_ref,
    keys, queries, part, pair_half, chip_half, line_in, line_half, middle_in, sums, triple,
    centred, squares, labels_ref, lists_ref, gain_ref, klist_ref, kgain_ref, kscale_ref,
    counts_ref, alpha, alpha_parts, products, acc_ref, cols_ref, returned_ref, rows_ref, rows_in,
    load_sems, stage_sems, z_sems, core_sems, key_sems, side_sems, relay_sems, flow_sems,
    scale_sems, return_sems, row_sems,
):
    dev = lax.axis_index("dev")
    group = lax.axis_index("outer")
    z, core = dev // 2, lax.rem(dev, 2)
    odd = lax.rem(group, 2)
    rows, width = docs_ref.shape
    span = width // PIECES
    half = PIECES // 2
    clusters = neighbours_ref.shape[1]
    base = group * 8
    partner_at = 2 * z + 1 - core
    partner = {"dev": partner_at}
    above = {"dev": lax.rem(dev + 2, 8)}
    below = {"dev": lax.rem(dev + 6, 8)}
    beside_group = group + 1 - 2 * odd
    opposite_group = 3 - group
    beside = {"outer": beside_group}
    opposite = {"outer": opposite_group}
    across = {"outer": lax.rem(group + 2, 4)}
    others = [lax.rem(dev + step, 8) for step in range(1, 8)]

    def loading(k):
        return pltpu.make_async_copy(
            docs_ref.at[:, pl.ds(pl.multiple_of(k * span, span), span)],
            keys.at[dev, k],
            load_sems.at[k],
        )

    loop(PIECES, lambda k: loading(k).start())
    barrier = pltpu.get_barrier_semaphore()
    peers = [{"dev": peer} for peer in others] + [beside, opposite, across]
    for peer in peers:
        pl.semaphore_signal(barrier, inc=1, device_id=peer, device_id_type=MESH)

    square = (rows, rows)
    same = lax.broadcasted_iota(jnp.int32, square, 0) == lax.broadcasted_iota(jnp.int32, square, 1)
    lane = lax.broadcasted_iota(jnp.int32, (1, 128), 1)

    def fetch_labels(slot, block):
        top = 3 * (block // 2)
        late = lax.rem(block, 2)
        first = cluster_ref[pl.ds(top, 1), :]
        middle = cluster_ref[pl.ds(top + 1, 1), :]
        last = cluster_ref[pl.ds(top + 2, 1), :]
        turned = jnp.where(lane < 64, pltpu.roll(middle, 64, 1), pltpu.roll(last, 64, 1))
        tail = jnp.where(late == 1, pltpu.roll(last, 64, 1), middle)
        labels_ref[slot, :, 0:128] = jnp.where(late == 1, turned, first)
        labels_ref[slot, :, 128:rows] = tail[:, 0 : rows - 128]

    loop(8, lambda at: fetch_labels(at, base + at))
    fetch_labels(8, beside_group * 8 + dev)
    fetch_labels(9, opposite_group * 8 + dev)
    own_labels = labels_ref[dev]
    member = (
        own_labels == base + lax.broadcasted_iota(jnp.int32, (8, rows), 0)
    ).astype(jnp.bfloat16)

    def partial_sums(k):
        loading(k).wait()
        part[k] = jnp.dot(member, keys[dev, k], preferred_element_type=jnp.float32)

    loop(PIECES, partial_sums)
    pl.semaphore_wait(barrier, len(peers))

    def remote(src, dst, send_sem, recv_sem, device):
        return pltpu.make_async_remote_copy(
            src_ref=src, dst_ref=dst, send_sem=send_sem, recv_sem=recv_sem,
            device_id=device, device_id_type=MESH,
        )

    def hop(unit, k, device):
        at = 2 * unit + core
        return remote(
            keys.at[at, k], keys.at[at, k], z_sems.at[unit], key_sems.at[at, k], device
        )

    def share(unit, k):
        at = 2 * unit + core
        return remote(
            keys.at[at, k], keys.at[at, k], core_sems.at[unit], key_sems.at[at, k], partner
        )

    def whole_sent(unit, sems):
        at = 2 * unit + core
        remote(keys.at[at], keys.at[at], sems.at[unit], key_sems.at[at, 0], partner).wait_send()

    def arrived(at, k):
        remote(
            keys.at[at, k], keys.at[at, k], core_sems.at[0], key_sems.at[at, k], partner
        ).wait_recv()

    def side(k):
        return remote(
            queries.at[k, 0], queries.at[k, 1], flow_sems.at[0], side_sems.at[k], beside
        )

    def relay(k):
        return remote(
            queries.at[k, 1], queries.at[k, 2], flow_sems.at[1], relay_sems.at[k], across
        )

    mine = pl.ds(pl.multiple_of(core * half, half), half)
    theirs = pl.ds(pl.multiple_of((1 - core) * half, half), half)

    def staged(n, src, dst, device):
        return remote(src, dst, stage_sems.at[n, 0], stage_sems.at[n, 1], device)

    pairing = staged(0, part.at[theirs], pair_half, partner)
    lower = staged(1, chip_half, line_in, above)
    upper = staged(1, chip_half, line_in, below)
    rising = staged(2, line_half, middle_in, above)
    sinking = staged(2, line_half, middle_in, below)
    outward_up = staged(3, sums.at[mine], sums.at[mine], above)
    outward_down = staged(3, sums.at[mine], sums.at[mine], below)
    joining = staged(4, sums.at[mine], sums.at[mine], partner)

    def own_hops(first, stop):
        def one(k):
            @pl.when(z < 2)
            def _():
                hop(z, k, above).start()

            @pl.when(z == 3)
            def _():
                hop(z, k, below).start()

        lax.fori_loop(first, stop, lambda k, carry: (one(k), carry)[1], 0)

    pairing.start()
    own_hops(0, 1)

    @pl.when(z == 1)
    def _():
        own_hops(1, 3)

    loop(PIECES, lambda k: share(z, k).start())
    pairing.wait_recv()
    chip_half[...] = part[mine] + pair_half[...]

    @pl.when(z == 0)
    def _():
        lower.start()

    @pl.when(z == 3)
    def _():
        upper.start()

    @pl.when((z == 0) | (z == 3))
    def _():
        own_hops(1, PIECES)

    @pl.when((z == 1) | (z == 2))
    def _():
        lower.wait_recv()
        line_half[...] = chip_half[...] + line_in[...]

        @pl.when(z == 1)
        def _():
            rising.start()
            own_hops(3, PIECES)

        @pl.when(z == 2)
        def _():
            sinking.start()

        rising.wait_recv()
        sums[mine] = line_half[...] + middle_in[...]

        @pl.when(z == 1)
        def _():
            outward_down.start()

        @pl.when(z == 2)
        def _():
            outward_up.start()

    @pl.when((z == 0) | (z == 3))
    def _():
        outward_up.wait_recv()

    joining.start()

    def chosen(read, labels, first, zero):
        found = jnp.full(labels.shape, zero, jnp.float32)
        for h in range(8):
            found = jnp.where(labels == first + h, read(first + h), found)
        return found

    def listed(position):
        return lambda c: neighbours_ref[position, c].astype(jnp.float32)

    def sharp(c):
        return sharpness_ref[c]

    def upright(row):
        return jnp.sum(jnp.where(same, row, 0.0), axis=1, keepdims=True)

    def flat(column):
        return jnp.sum(jnp.where(same, column, 0.0), axis=0, keepdims=True)

    def count_of(c):
        hits = jnp.where(cluster_ref[...] == c, 1.0, 0.0)
        return jnp.sum(jnp.sum(hits, axis=0, keepdims=True), axis=1, keepdims=True)

    own_row = own_labels.astype(jnp.float32)
    own_upright = upright(own_row)
    lists_ref[0, 0] = own_upright
    upright_member = (
        own_upright
        == base.astype(jnp.float32)
        + lax.rem(lax.broadcasted_iota(jnp.int32, (rows, 24), 1), 8).astype(jnp.float32)
    ).astype(jnp.bfloat16)
    local = lax.broadcasted_iota(jnp.int32, (8, 1), 0)
    own_sizes = jnp.zeros((8, 1), jnp.float32)
    for h in range(8):
        own_sizes = jnp.where(local == h, count_of(base + h), own_sizes)

    acc_ref[...] = jnp.zeros_like(acc_ref)

    alpha[...] = jnp.zeros_like(alpha)
    products[...] = jnp.zeros_like(products)
    joining.wait_recv()
    squares[...] = jnp.zeros_like(squares)

    def centre_piece(k):
        means = sums[k] / own_sizes
        high = means.astype(jnp.bfloat16).astype(jnp.float32)
        rest = means - high
        mid = rest.astype(jnp.bfloat16).astype(jnp.float32)
        parts = jnp.concatenate([high, mid, rest - mid], axis=0).astype(jnp.bfloat16)
        triple[k] = parts
        centre = jnp.dot(upright_member, parts, preferred_element_type=jnp.float32)
        moved = keys[dev, k].astype(jnp.float32) - centre
        centred[k] = moved
        squares[...] += moved * moved

    loop(PIECES, centre_piece)
    energy = jnp.sum(squares[...], axis=1, keepdims=True) / width
    scaling = lax.rsqrt(energy + 1e-06) / math.sqrt(width)

    def unit_piece(k):
        queries[k, 0] = (centred[k] * scaling).astype(jnp.bfloat16)

        @pl.when(k > 0)
        def _():
            side(k - 1).start()

    loop(PIECES, unit_piece)
    kscale_ref[dev] = flat(scaling)
    side(PIECES - 1).start()

    def scale_out(n):
        return remote(
            kscale_ref.at[dev], kscale_ref.at[dev],
            scale_sems.at[0, n], scale_sems.at[1, dev], {"dev": others[n]},
        )

    for n in range(7):
        scale_out(n).start()

    def onward(k):
        @pl.when(z == 1)
        def _():
            arrived(core, k)
            hop(0, k, above).start()
            share(0, k).start()

        @pl.when(z == 2)
        def _():
            arrived(6 + core, k)
            hop(3, k, below).start()
            share(3, k).start()
            arrived(2 + core, k)
            share(1, k).start()

    contract = (((1,), (1,)), ((), ()))

    def stacked(k):
        return queries[k].reshape(3 * rows, span)

    def multiply(at, first, count):
        found = [
            lax.dot_general(
                stacked(first + k), keys[at, first + k], contract,
                preferred_element_type=jnp.float32,
            )
            for k in range(count)
        ]
        products[at] += functools.reduce(jnp.add, found)

    early = jnp.where(z == 2, 3, jnp.where(z == 1, 2, 1))

    def early_unit(n):
        return jnp.where(n == 0, z, jnp.where(n == 2, 3, z - 1))

    def absorb(first):
        for k in range(GROUPED):
            relay(first + k).wait_recv()
        alpha[...] += functools.reduce(
            jnp.add,
            [
                lax.dot_general(
                    stacked(first + k), triple[first + k], contract,
                    preferred_element_type=jnp.float32,
                )
                for k in range(GROUPED)
            ],
        )

    def consume(n, first):
        unit = early_unit(n)
        multiply(2 * unit + core, first, GROUPED)
        for k in range(GROUPED):
            arrived(2 * unit + 1 - core, first + k)
        multiply(2 * unit + 1 - core, first, GROUPED)

    def query_tables():
        for b, slot in ((0, dev), (1, 8), (2, 9)):
            first = (base, beside_group * 8, opposite_group * 8)[b]
            labels = labels_ref[slot]
            if b > 0:
                lists_ref[b, 0] = upright(labels.astype(jnp.float32))
            gain_ref[b] = upright(chosen(sharp, labels, first, 0.0))
            positions = ((0, 1), (2 + odd,), (3 - odd,))[b]
            for place, position in enumerate(positions):
                lists_ref[b, 1 + place] = upright(chosen(listed(position), labels, first, 0.0))

    def all_key_tables():
        def key_tables(at):
            labels = labels_ref[at]
            klist_ref[at, 0] = labels.astype(jnp.float32)
            kgain_ref[at] = chosen(sharp, labels, base, 0.0)
            klist_ref[at, 1] = chosen(listed(3 - odd), labels, base, 0.0)
            klist_ref[at, 2] = chosen(listed(2 + odd), labels, base, 0.0)

        loop(8, key_tables)
    def count_table():
        own_lists = [chosen(listed(position), own_labels, base, 0.0) for position in range(4)]

        def add_count(c, total):
            here = c.astype(jnp.float32)
            found = jnp.where(own_row == here, 1.0, 0.0)
            for row in own_lists:
                found = found + jnp.where(row == here, 1.0, 0.0)
            return total + found * count_of(c)

        counts_ref[...] = lax.fori_loop(0, clusters, add_count, jnp.full((1, rows), -1.0, jnp.float32))

    def steps(k):
        @pl.when(k < PIECES)
        def _():
            side(k).wait_recv()
            relay(k).start()

        @pl.when(k < half)
        def _():
            onward(2 * k)
            onward(2 * k + 1)

        @pl.when((z == 1) & (k > 1) & (k < PIECES + 2))
        def _():
            arrived(6 + core, k - 2)
            hop(3, k - 2, below).start()
            share(3, k - 2).start()

        for when, table in ((1, query_tables), (2, all_key_tables), (3, count_table)):
            pl.when(k == when)(table)

        turn = lax.rem(k - 1, GROUPED)
        first = k - 1 - turn - GROUPED

        @pl.when((first >= 0) & (turn == 0))
        def _():
            absorb(first)

        @pl.when((first >= 0) & (turn < early))
        def _():
            consume(turn, first)

    loop(PIECES + GROUPED, steps)
    high = alpha[...].astype(jnp.bfloat16)
    rest = alpha[...] - high.astype(jnp.float32)
    mid = rest.astype(jnp.bfloat16)
    alpha_parts[:, 0:24] = high
    alpha_parts[:, 24:48] = mid
    alpha_parts[:, 48:72] = (rest - mid.astype(jnp.float32)).astype(jnp.bfloat16)
    cluster_of_part = base + lax.rem(lax.broadcasted_iota(jnp.int32, (72, rows), 0), 8)

    def settle(at):
        hot = (labels_ref[at] == cluster_of_part).astype(jnp.bfloat16)
        products[at] -= jnp.dot(alpha_parts[...], hot, preferred_element_type=jnp.float32)

    def finish(at):
        @pl.when(at != dev)
        def _():
            remote(
                kscale_ref.at[at], kscale_ref.at[at],
                scale_sems.at[0, 0], scale_sems.at[1, at], partner,
            ).wait_recv()

        down = jnp.zeros((1, rows), jnp.float32)
        kl = klist_ref[at, 0]
        scale = 0.5 * kscale_ref[at]
        for b in range(3):
            terms = jnp.exp(
                (gain_ref[b] + kgain_ref[at]) * (scale * products[at, pl.ds(b * rows, rows), :])
            )
            wanted = lists_ref[b, 1] == kl
            if b == 0:
                wanted = wanted | (lists_ref[0, 2] == kl) | (lists_ref[0, 0] == kl)
                wanted = wanted & jnp.logical_not(same & (at == dev))
                back = wanted
            else:
                back = lists_ref[b, 0] == klist_ref[at, b]
            acc_ref[b] += jnp.where(wanted, terms, 0.0)
            down = down + jnp.sum(jnp.where(back, terms, 0.0), axis=0, keepdims=True)
        cols_ref[at] = down

    def give_back(at):
        return remote(
            cols_ref.at[at], returned_ref.at[dev],
            return_sems.at[0, at], return_sems.at[1, dev], {"dev": at},
        )

    def finish_early(n):
        unit = early_unit(n)

        def one(c):
            settle(2 * unit + c)
            finish(2 * unit + c)

        loop(2, one)

        @pl.when(n > 0)
        def _():
            loop(2, lambda c: give_back(2 * unit + c).start())

    loop(early, finish_early)

    @pl.when(z < 3)
    def _():
        unit = jnp.where(z == 2, 0, 3)
        ours, other = 2 * unit + core, 2 * unit + 1 - core
        settle(ours)
        settle(other)

        def stream(first, count):
            @pl.when(z != 1)
            def _():
                for k in range(count):
                    arrived(ours, first + k)
                    share(unit, first + k).start()

            multiply(ours, first, count)
            for k in range(count):
                arrived(other, first + k)
            multiply(other, first, count)

        loop(PIECES // GROUPED - 1, lambda g: stream(g * GROUPED, GROUPED))
        stream(PIECES - GROUPED, GROUPED - 1)
        stream(PIECES - 1, 1)
        finish(ours)
        give_back(ours).start()
        finish(other)
        give_back(other).start()

    def row_back(b, device):
        return remote(
            rows_ref.at[b], rows_in.at[b - 1], row_sems.at[0, b - 1], row_sems.at[1, b - 1], device
        )

    for b in (2, 1, 0):
        rows_ref[b] = flat(jnp.sum(acc_ref[b], axis=1, keepdims=True))
        if b > 0:
            row_back(b, {1: beside, 2: opposite}[b]).start()

    def came_back(sender):
        remote(
            cols_ref.at[0], returned_ref.at[sender],
            return_sems.at[0, 0], return_sems.at[1, sender], partner,
        ).wait_recv()

    cols_ref[dev] = rows_ref[0]

    def collect(sender):
        unit = sender // 2
        gives = (
            ((z == 0) & ((unit == 1) | (unit == 2)))
            | ((z == 1) & (unit == 2))
            | ((z == 3) & (unit < 3))
        )

        @pl.when(gives)
        def _():
            came_back(sender)
            cols_ref[dev] += returned_ref[sender]

    loop(8, collect)
    row_back(1, beside).wait_recv()
    row_back(2, opposite).wait_recv()
    total = cols_ref[dev] + rows_in[0] + rows_in[1]
    out_ref[...] = jnp.log(total / counts_ref[...])

    pairing.wait_send()
    joining.wait_send()
    whole_sent(z, core_sems)
    remote(queries.at[:, 0], queries.at[:, 1], flow_sems.at[0], side_sems.at[0], beside).wait_send()
    remote(queries.at[:, 1], queries.at[:, 2], flow_sems.at[1], relay_sems.at[0], across).wait_send()
    row_back(1, beside).wait_send()
    row_back(2, opposite).wait_send()
    for n in range(7):
        scale_out(n).wait_send()

    def scale_rest(at):
        unit = at // 2
        used = (
            (unit == z)
            | ((z == 0) & (unit == 3))
            | ((z == 1) & ((unit == 0) | (unit == 3)))
            | ((z == 2) & ((unit == 0) | (unit == 1) | (unit == 3)))
        )

        @pl.when(jnp.logical_not(used))
        def _():
            remote(
                kscale_ref.at[at], kscale_ref.at[at],
                scale_sems.at[0, 0], scale_sems.at[1, at], partner,
            ).wait_recv()

    loop(8, scale_rest)

    def returns_sent(unit):
        loop(2, lambda c: give_back(2 * unit + c).wait_send())

    @pl.when(z != 2)
    def _():
        whole_sent(z, z_sems)

    @pl.when((z == 0) | (z == 3))
    def _():
        lower.wait_send()

    @pl.when((z == 1) | (z == 2))
    def _():
        rising.wait_send()
        outward_up.wait_send()

    @pl.when(z == 0)
    def _():
        whole_sent(3, core_sems)
        returns_sent(3)

    @pl.when(z == 1)
    def _():
        whole_sent(0, z_sems)
        whole_sent(3, z_sems)
        whole_sent(0, core_sems)
        whole_sent(3, core_sems)
        returns_sent(0)
        returns_sent(3)

    @pl.when(z == 2)
    def _():
        whole_sent(3, z_sems)
        for unit in (0, 1, 3):
            whole_sent(unit, core_sems)
            returns_sent(unit)


def gathered(documents, cluster_of, neighbours, sharpness):
    rows, width = documents.shape
    span = width // PIECES
    half = PIECES // 2
    vmem = pl.BlockSpec(memory_space=pltpu.VMEM)
    smem = pl.BlockSpec(memory_space=pltpu.SMEM)
    f32 = functools.partial(pltpu.VMEM, dtype=jnp.float32)
    bf16 = functools.partial(pltpu.VMEM, dtype=jnp.bfloat16)
    sems = pltpu.SemaphoreType.DMA
    density = pl.pallas_call(
        density_kernel,
        out_shape=jax.ShapeDtypeStruct((1, rows), jnp.float32),
        in_specs=[pl.BlockSpec(memory_space=pl.ANY), vmem, smem, smem],
        out_specs=vmem,
        scratch_shapes=[
            bf16((8, PIECES, rows, span)),
            bf16((PIECES, 3, rows, span)),
            f32((PIECES, 8, span)),
            f32((half, 8, span)),
            f32((half, 8, span)),
            f32((half, 8, span)),
            f32((half, 8, span)),
            f32((half, 8, span)),
            f32((PIECES, 8, span)),
            bf16((PIECES, 24, span)),
            f32((PIECES, rows, span)),
            f32((rows, span)),
            pltpu.VMEM((10, 1, rows), jnp.int32),
            f32((3, 3, rows, 1)),
            f32((3, rows, 1)),
            f32((8, 3, 1, rows)),
            f32((8, 1, rows)),
            f32((8, 1, rows)),
            f32((1, rows)),
            f32((3 * rows, 24)),
            bf16((3 * rows, 72)),
            f32((8, 3 * rows, rows)),
            f32((3, rows, rows)),
            f32((8, 1, rows)),
            f32((8, 1, rows)),
            f32((3, 1, rows)),
            f32((2, 1, rows)),
            sems((PIECES,)),
            sems((5, 2)),
            sems((4,)),
            sems((4,)),
            sems((8, PIECES)),
            sems((PIECES,)),
            sems((PIECES,)),
            sems((2,)),
            sems((2, 8)),
            sems((2, 8)),
            sems((2, 2)),
        ],
        compiler_params=pltpu.CompilerParams(
            collective_id=0, has_side_effects=True, vmem_limit_bytes=56 * 1024 * 1024
        ),
        name="density",
    )(documents, cluster_of.reshape(-1, 128), neighbours.T, sharpness)
    return density.reshape(rows)


def solution(mesh):
    small = mesh.shape["dev"] == 8 and mesh.shape["outer"] == 4
    in_specs = (P(("outer", "dev"), None), P(), P(), P())
    out_specs = P(("outer", "dev"))
    body = gathered if small else shards
    return jax.shard_map(body, mesh=mesh, in_specs=in_specs, out_specs=out_specs, check_vma=False)
```

```python
import functools
import math

import jax
import jax.numpy as jnp
from jax import lax
from jax.experimental import pallas as pl
from jax.experimental.pallas import tpu as pltpu
from jax.sharding import PartitionSpec as P


def passed_along(block, axis, distance):
    devices = range(lax.axis_size(axis))
    route = [((i - distance) % len(devices), i) for i in devices]
    return lax.ppermute(block, axis, route)


def kernel_block(queries, others, pair_gain):
    products = jnp.einsum("qe,ke->qk", queries, others, preferred_element_type=jnp.float32)
    return jnp.exp(pair_gain * products)


def shards(documents, cluster_of, neighbours, sharpness):
    groups = lax.axis_size("outer")
    owners = lax.axis_size("dev")
    tokens_here = documents.shape[0]
    feature_width = documents.shape[1]
    capacity = max(2, 2 * tokens_here // owners)
    slot_count = owners * capacity
    group_index = lax.axis_index("outer")
    owner_index = lax.axis_index("dev")
    own_cluster = group_index * owners + owner_index
    block_labels = cluster_of.reshape(groups * owners, tokens_here)
    group_of_block = jnp.arange(groups * owners, dtype=jnp.int32) // owners
    local_labels = block_labels - group_of_block[:, None] * owners
    owner_range = jnp.arange(owners, dtype=jnp.int32)
    per_block = jnp.sum(
        (local_labels[:, :, None] == owner_range).astype(jnp.int32), axis=1
    ).reshape(groups, owners, owners)
    cluster_sizes = jnp.sum(per_block, axis=1).reshape(-1)
    own_labels = lax.dynamic_index_in_dim(local_labels, own_cluster, 0, keepdims=False)
    ordinal = jnp.arange(tokens_here, dtype=jnp.int32)
    earlier = ordinal[None, :] < ordinal[:, None]
    repeats = jnp.sum(
        ((own_labels[:, None] == own_labels[None, :]) & earlier).astype(jnp.int32), axis=1
    )
    target = own_labels * capacity + repeats
    placing = (jnp.arange(slot_count, dtype=jnp.int32)[:, None] == target[None, :]).astype(
        jnp.bfloat16
    )
    outgoing = jnp.dot(placing, documents, preferred_element_type=jnp.float32).astype(jnp.bfloat16)
    arrived = lax.all_to_all(
        outgoing.reshape(owners, capacity, feature_width),
        "dev",
        split_axis=0,
        concat_axis=0,
        tiled=True,
    ).reshape(slot_count, feature_width)

    def slot_mask(group_at, owner_at):
        senders = per_block[group_at, :, owner_at]
        return (
            (jnp.arange(capacity, dtype=jnp.int32)[None, :] < senders[:, None])
            .astype(jnp.float32)
            .reshape(-1)
        )

    present = slot_mask(group_index, owner_index)
    centre = jnp.dot(
        present.astype(jnp.bfloat16)[None, :], arrived, preferred_element_type=jnp.float32
    )[0]
    centre = centre / cluster_sizes[own_cluster].astype(jnp.float32)
    centred = arrived.astype(jnp.float32) - centre[None, :]
    scaling = lax.rsqrt(jnp.mean(centred * centred, axis=1) + 1e-06) / math.sqrt(feature_width)
    unit_rows = (centred * (scaling * present)[:, None]).astype(jnp.bfloat16)
    own_gain = sharpness[own_cluster]
    listed = neighbours[own_cluster]
    off_diagonal = 1.0 - jnp.eye(slot_count, dtype=jnp.float32)
    running = jnp.sum(
        kernel_block(unit_rows, unit_rows, own_gain) * (present[None, :] * off_diagonal), axis=1
    )
    beside = [passed_along(unit_rows, "dev", offset) for offset in (1, -1)]
    vertical = []
    for direction, position in ((1, 2), (-1, 3)):
        receiver_group = (group_index + direction) % groups
        wanted = neighbours[receiver_group * owners + owner_index, position]
        delta = (wanted % owners - owner_index + owners) % owners
        picked_rows = jnp.where(
            delta == 1, beside[1], jnp.where(delta == owners - 1, beside[0], unit_rows)
        )
        vertical.append(passed_along(picked_rows, "outer", direction))
    key_sets = [beside[0], beside[1], vertical[0], vertical[1]]
    for position in range(4):
        partner = listed[position]
        partner_group_at = partner // owners
        partner_owner_at = partner % owners
        partner_partner = partner_group_at * owners + partner_owner_at
        pair_gain = 0.5 * (own_gain + sharpness[partner_partner])
        partner = partner_partner
        kernel_terms = kernel_block(unit_rows, key_sets[position], pair_gain)
        key_mask = slot_mask(partner_group_at, partner_owner_at)
        running = running + jnp.sum(kernel_terms * key_mask[None, :], axis=1)
    partner_count = cluster_sizes[own_cluster] - 1 + jnp.sum(cluster_sizes[listed])
    slot_density = jnp.log(running / partner_count.astype(jnp.float32))
    answered = lax.all_to_all(
        slot_density.reshape(owners, capacity), "dev", split_axis=0, concat_axis=0, tiled=True
    ).reshape(-1)
    return answered[target]


MESH = pl.DeviceIdType.MESH


PIECES = 16
GROUPED = 4


def start(copy):
    copy.start()


def sent(copy):
    copy.wait_send()


def landed(copy):
    copy.wait_recv()


def loop(count, body):
    lax.fori_loop(0, count, lambda k, carry: (body(k), carry)[1], 0)


def density_kernel(
    docs_ref, cluster_ref, neighbours_ref, sharpness_ref, out_ref,
    keys, queries, part, pair_half, chip_half, line_in, line_half, middle_in, sums, triple,
    centred, squares, labels_ref, lists_ref, gain_ref, klist_ref, kgain_ref, kscale_ref,
    counts_ref, alpha, alpha_parts, products, acc_ref, cols_ref, returned_ref, rows_ref, rows_in,
    load_sems, stage_sems, z_sems, core_sems, key_sems, side_sems, relay_sems, flow_sems,
    scale_sems, return_sems, row_sems,
):
    dev = lax.axis_index("dev")
    group = lax.axis_index("outer")
    z, core = dev // 2, lax.rem(dev, 2)
    odd = lax.rem(group, 2)
    rows, width = docs_ref.shape
    span = width // PIECES
    half = PIECES // 2
    clusters = neighbours_ref.shape[1]
    base = group * 8
    partner_at = 2 * z + 1 - core
    partner = {"dev": partner_at}
    above = {"dev": lax.rem(dev + 2, 8)}
    below = {"dev": lax.rem(dev + 6, 8)}
    beside_group = group + 1 - 2 * odd
    opposite_group = 3 - group
    beside = {"outer": beside_group}
    opposite = {"outer": opposite_group}
    across = {"outer": lax.rem(group + 2, 4)}
    others = [lax.rem(dev + step, 8) for step in range(1, 8)]

    def loading(k):
        return pltpu.make_async_copy(
            docs_ref.at[:, pl.ds(pl.multiple_of(k * span, span), span)],
            keys.at[dev, k],
            load_sems.at[k],
        )

    loop(PIECES, lambda k: loading(k).start())
    barrier = pltpu.get_barrier_semaphore()
    peers = [{"dev": peer} for peer in others] + [beside, opposite, across]
    for peer in peers:
        pl.semaphore_signal(barrier, inc=1, device_id=peer, device_id_type=MESH)

    square = (rows, rows)
    same = lax.broadcasted_iota(jnp.int32, square, 0) == lax.broadcasted_iota(jnp.int32, square, 1)
    lane = lax.broadcasted_iota(jnp.int32, (1, 128), 1)

    def fetch_labels(slot, block):
        top = 3 * (block // 2)
        late = lax.rem(block, 2)
        first = cluster_ref[pl.ds(top, 1), :]
        middle = cluster_ref[pl.ds(top + 1, 1), :]
        last = cluster_ref[pl.ds(top + 2, 1), :]
        turned = jnp.where(lane < 64, pltpu.roll(middle, 64, 1), pltpu.roll(last, 64, 1))
        tail = jnp.where(late == 1, pltpu.roll(last, 64, 1), middle)
        labels_ref[slot, :, 0:128] = jnp.where(late == 1, turned, first)
        labels_ref[slot, :, 128:rows] = tail[:, 0 : rows - 128]

    loop(8, lambda at: fetch_labels(at, base + at))
    fetch_labels(8, beside_group * 8 + dev)
    fetch_labels(9, opposite_group * 8 + dev)
    own_labels = labels_ref[dev]
    member = (
        own_labels == base + lax.broadcasted_iota(jnp.int32, (8, rows), 0)
    ).astype(jnp.bfloat16)

    def partial_sums(k):
        loading(k).wait()
        part[k] = jnp.dot(member, keys[dev, k], preferred_element_type=jnp.float32)

    loop(PIECES, partial_sums)
    pl.semaphore_wait(barrier, len(peers))

    def remote(src, dst, send_sem, recv_sem, device):
        return pltpu.make_async_remote_copy(
            src_ref=src, dst_ref=dst, send_sem=send_sem, recv_sem=recv_sem,
            device_id=device, device_id_type=MESH,
        )

    def hop(unit, k, device):
        at = 2 * unit + core
        return remote(
            keys.at[at, k], keys.at[at, k], z_sems.at[unit], key_sems.at[at, k], device
        )

    def share(unit, k):
        at = 2 * unit + core
        return remote(
            keys.at[at, k], keys.at[at, k], core_sems.at[unit], key_sems.at[at, k], partner
        )

    def whole_sent(unit, sems):
        at = 2 * unit + core
        remote(keys.at[at], keys.at[at], sems.at[unit], key_sems.at[at, 0], partner).wait_send()

    def arrived(at, k):
        remote(
            keys.at[at, k], keys.at[at, k], core_sems.at[0], key_sems.at[at, k], partner
        ).wait_recv()

    def side(k):
        return remote(
            queries.at[k, 0], queries.at[k, 1], flow_sems.at[0], side_sems.at[k], beside
        )

    def relay(k):
        return remote(
            queries.at[k, 1], queries.at[k, 2], flow_sems.at[1], relay_sems.at[k], across
        )

    mine = pl.ds(pl.multiple_of(core * half, half), half)
    theirs = pl.ds(pl.multiple_of((1 - core) * half, half), half)

    def staged(n, src, dst, device):
        return remote(src, dst, stage_sems.at[n, 0], stage_sems.at[n, 1], device)

    pairing = staged(0, part.at[theirs], pair_half, partner)
    lower = staged(1, chip_half, line_in, above)
    upper = staged(1, chip_half, line_in, below)
    rising = staged(2, line_half, middle_in, above)
    sinking = staged(2, line_half, middle_in, below)
    outward_up = staged(3, sums.at[mine], sums.at[mine], above)
    outward_down = staged(3, sums.at[mine], sums.at[mine], below)
    joining = staged(4, sums.at[mine], sums.at[mine], partner)

    def own_hops(first, stop):
        def one(k):
            @pl.when(z < 3)
            def _():
                hop(z, k, above).start()

            @pl.when(z == 3)
            def _():
                hop(z, k, below).start()

        lax.fori_loop(first, stop, lambda k, carry: (one(k), carry)[1], 0)

    pairing.start()

    @pl.when(z != 2)
    def _():
        own_hops(0, 1)

    @pl.when(z == 1)
    def _():
        own_hops(1, 3)

    loop(PIECES, lambda k: share(z, k).start())
    pairing.wait_recv()
    chip_half[...] = part[mine] + pair_half[...]

    @pl.when(z == 0)
    def _():
        lower.start()

    @pl.when(z == 3)
    def _():
        upper.start()

    @pl.when((z == 0) | (z == 3))
    def _():
        own_hops(1, PIECES)

    @pl.when((z == 1) | (z == 2))
    def _():
        lower.wait_recv()
        line_half[...] = chip_half[...] + line_in[...]

        @pl.when(z == 1)
        def _():
            rising.start()
            own_hops(3, PIECES)

        @pl.when(z == 2)
        def _():
            sinking.start()

        rising.wait_recv()
        sums[mine] = line_half[...] + middle_in[...]

        @pl.when(z == 1)
        def _():
            outward_down.start()

        @pl.when(z == 2)
        def _():
            outward_up.start()
            own_hops(0, PIECES)

    @pl.when((z == 0) | (z == 3))
    def _():
        outward_up.wait_recv()

    joining.start()

    def chosen(read, labels, first, zero):
        found = jnp.full(labels.shape, zero, jnp.float32)
        for h in range(8):
            found = jnp.where(labels == first + h, read(first + h), found)
        return found

    def listed(position):
        return lambda c: neighbours_ref[position, c].astype(jnp.float32)

    def sharp(c):
        return sharpness_ref[c]

    def upright(row):
        return jnp.sum(jnp.where(same, row, 0.0), axis=1, keepdims=True)

    def flat(column):
        return jnp.sum(jnp.where(same, column, 0.0), axis=0, keepdims=True)

    def count_of(c):
        hits = jnp.where(cluster_ref[...] == c, 1.0, 0.0)
        return jnp.sum(jnp.sum(hits, axis=0, keepdims=True), axis=1, keepdims=True)

    own_row = own_labels.astype(jnp.float32)
    own_upright = upright(own_row)
    lists_ref[0, 0] = own_upright
    upright_member = (
        own_upright
        == base.astype(jnp.float32)
        + lax.rem(lax.broadcasted_iota(jnp.int32, (rows, 24), 1), 8).astype(jnp.float32)
    ).astype(jnp.bfloat16)
    local = lax.broadcasted_iota(jnp.int32, (8, 1), 0)
    own_sizes = jnp.zeros((8, 1), jnp.float32)
    for h in range(8):
        own_sizes = jnp.where(local == h, count_of(base + h), own_sizes)

    acc_ref[...] = jnp.zeros_like(acc_ref)

    alpha[...] = jnp.zeros_like(alpha)
    products[...] = jnp.zeros_like(products)
    joining.wait_recv()
    squares[...] = jnp.zeros_like(squares)

    def centre_piece(k):
        means = sums[k] / own_sizes
        high = means.astype(jnp.bfloat16).astype(jnp.float32)
        rest = means - high
        mid = rest.astype(jnp.bfloat16).astype(jnp.float32)
        parts = jnp.concatenate([high, mid, rest - mid], axis=0).astype(jnp.bfloat16)
        triple[k] = parts
        centre = jnp.dot(upright_member, parts, preferred_element_type=jnp.float32)
        moved = keys[dev, k].astype(jnp.float32) - centre
        centred[k] = moved
        squares[...] += moved * moved

    loop(PIECES, centre_piece)
    energy = jnp.sum(squares[...], axis=1, keepdims=True) / width
    scaling = lax.rsqrt(energy + 1e-06) / math.sqrt(width)

    def unit_piece(k):
        queries[k, 0] = (centred[k] * scaling).astype(jnp.bfloat16)

        @pl.when(k > 0)
        def _():
            side(k - 1).start()

    loop(PIECES, unit_piece)
    kscale_ref[dev] = flat(scaling)
    side(PIECES - 1).start()

    def scale_out(n):
        return remote(
            kscale_ref.at[dev], kscale_ref.at[dev],
            scale_sems.at[0, n], scale_sems.at[1, dev], {"dev": others[n]},
        )

    for n in range(7):
        scale_out(n).start()

    def onward(k):
        @pl.when(z == 1)
        def _():
            arrived(core, k)
            hop(0, k, above).start()
            share(0, k).start()

        @pl.when(z == 2)
        def _():
            arrived(6 + core, k)
            hop(3, k, below).start()
            arrived(2 + core, k)
            share(1, k).start()

    contract = (((1,), (1,)), ((), ()))

    def stacked(k):
        return queries[k].reshape(3 * rows, span)

    def multiply(at, first, count):
        found = [
            lax.dot_general(
                stacked(first + k), keys[at, first + k], contract,
                preferred_element_type=jnp.float32,
            )
            for k in range(count)
        ]
        products[at] += functools.reduce(jnp.add, found)

    early = jnp.where(z > 0, 2, 1)

    def early_unit(n):
        return z - n

    def absorb(first):
        for k in range(GROUPED):
            relay(first + k).wait_recv()
        alpha[...] += functools.reduce(
            jnp.add,
            [
                lax.dot_general(
                    stacked(first + k), triple[first + k], contract,
                    preferred_element_type=jnp.float32,
                )
                for k in range(GROUPED)
            ],
        )

    def consume(n, first):
        unit = early_unit(n)
        multiply(2 * unit + core, first, GROUPED)
        for k in range(GROUPED):
            arrived(2 * unit + 1 - core, first + k)
        multiply(2 * unit + 1 - core, first, GROUPED)

    last = jnp.where(z == 2, 0, 3)
    ours, other = 2 * last + core, 2 * last + 1 - core

    def stream(first, count):
        @pl.when(z != 1)
        def _():
            for k in range(count):
                arrived(ours, first + k)
                share(last, first + k).start()

        multiply(ours, first, count)
        for k in range(count):
            arrived(other, first + k)
        multiply(other, first, count)

    def query_tables():
        for b, slot in ((0, dev), (1, 8), (2, 9)):
            first = (base, beside_group * 8, opposite_group * 8)[b]
            labels = labels_ref[slot]
            if b > 0:
                lists_ref[b, 0] = upright(labels.astype(jnp.float32))
            gain_ref[b] = upright(chosen(sharp, labels, first, 0.0))
            positions = ((0, 1), (2 + odd,), (3 - odd,))[b]
            for place, position in enumerate(positions):
                lists_ref[b, 1 + place] = upright(chosen(listed(position), labels, first, 0.0))

    def all_key_tables():
        def key_tables(at):
            labels = labels_ref[at]
            klist_ref[at, 0] = labels.astype(jnp.float32)
            kgain_ref[at] = chosen(sharp, labels, base, 0.0)
            klist_ref[at, 1] = chosen(listed(3 - odd), labels, base, 0.0)
            klist_ref[at, 2] = chosen(listed(2 + odd), labels, base, 0.0)

        loop(8, key_tables)
    def count_table():
        own_lists = [chosen(listed(position), own_labels, base, 0.0) for position in range(4)]

        def add_count(c, total):
            here = c.astype(jnp.float32)
            found = jnp.where(own_row == here, 1.0, 0.0)
            for row in own_lists:
                found = found + jnp.where(row == here, 1.0, 0.0)
            return total + found * count_of(c)

        counts_ref[...] = lax.fori_loop(0, clusters, add_count, jnp.full((1, rows), -1.0, jnp.float32))

    def steps(k):
        @pl.when(k < PIECES)
        def _():
            side(k).wait_recv()
            relay(k).start()

        @pl.when(k < half)
        def _():
            onward(2 * k)
            onward(2 * k + 1)

        @pl.when((z == 3) & (k < PIECES))
        def _():
            arrived(4 + core, k)
            share(2, k).start()

        @pl.when((z == 1) & (k > 1) & (k < PIECES + 2))
        def _():
            arrived(6 + core, k - 2)
            hop(3, k - 2, below).start()
            share(3, k - 2).start()

        for when, table in ((1, query_tables), (2, all_key_tables), (3, count_table)):
            pl.when(k == when)(table)

        turn = lax.rem(k - 1, GROUPED)
        first = k - 1 - turn - GROUPED

        @pl.when((first >= 0) & (turn == 0))
        def _():
            absorb(first)

        @pl.when((first >= 0) & (turn < early))
        def _():
            consume(turn, first)

        @pl.when((z == 2) & (k == PIECES - 1))
        def _():
            stream(0, GROUPED)

    loop(PIECES + GROUPED, steps)
    high = alpha[...].astype(jnp.bfloat16)
    rest = alpha[...] - high.astype(jnp.float32)
    mid = rest.astype(jnp.bfloat16)
    alpha_parts[:, 0:24] = high
    alpha_parts[:, 24:48] = mid
    alpha_parts[:, 48:72] = (rest - mid.astype(jnp.float32)).astype(jnp.bfloat16)
    cluster_of_part = base + lax.rem(lax.broadcasted_iota(jnp.int32, (72, rows), 0), 8)

    def settle(at):
        hot = (labels_ref[at] == cluster_of_part).astype(jnp.bfloat16)
        products[at] -= jnp.dot(alpha_parts[...], hot, preferred_element_type=jnp.float32)

    def finish(at):
        @pl.when(at != dev)
        def _():
            remote(
                kscale_ref.at[at], kscale_ref.at[at],
                scale_sems.at[0, 0], scale_sems.at[1, at], partner,
            ).wait_recv()

        down = jnp.zeros((1, rows), jnp.float32)
        kl = klist_ref[at, 0]
        scale = 0.5 * kscale_ref[at]
        for b in range(3):
            terms = jnp.exp(
                (gain_ref[b] + kgain_ref[at]) * (scale * products[at, pl.ds(b * rows, rows), :])
            )
            wanted = lists_ref[b, 1] == kl
            if b == 0:
                wanted = wanted | (lists_ref[0, 2] == kl) | (lists_ref[0, 0] == kl)
                wanted = wanted & jnp.logical_not(same & (at == dev))
                back = wanted
            else:
                back = lists_ref[b, 0] == klist_ref[at, b]
            acc_ref[b] += jnp.where(wanted, terms, 0.0)
            down = down + jnp.sum(jnp.where(back, terms, 0.0), axis=0, keepdims=True)
        cols_ref[at] = down

    def give_back(at):
        return remote(
            cols_ref.at[at], returned_ref.at[dev],
            return_sems.at[0, at], return_sems.at[1, dev], {"dev": at},
        )

    def finish_early(n):
        unit = early_unit(n)

        def one(c):
            settle(2 * unit + c)
            finish(2 * unit + c)

        loop(2, one)

        @pl.when(n > 0)
        def _():
            loop(2, lambda c: give_back(2 * unit + c).start())

    loop(early, finish_early)

    @pl.when(z < 3)
    def _():
        settle(ours)
        settle(other)

        lax.fori_loop(
            jnp.where(z == 2, 1, 0), PIECES // GROUPED - 1,
            lambda g, carry: (stream(g * GROUPED, GROUPED), carry)[1], 0,
        )
        stream(PIECES - GROUPED, GROUPED - 1)
        stream(PIECES - 1, 1)
        finish(ours)
        give_back(ours).start()
        finish(other)
        give_back(other).start()

    def row_back(b, device):
        return remote(
            rows_ref.at[b], rows_in.at[b - 1], row_sems.at[0, b - 1], row_sems.at[1, b - 1], device
        )

    for b in (2, 1, 0):
        rows_ref[b] = flat(jnp.sum(acc_ref[b], axis=1, keepdims=True))
        if b > 0:
            row_back(b, {1: beside, 2: opposite}[b]).start()

    def came_back(sender):
        remote(
            cols_ref.at[0], returned_ref.at[sender],
            return_sems.at[0, 0], return_sems.at[1, sender], partner,
        ).wait_recv()

    cols_ref[dev] = rows_ref[0]

    def collect(sender):
        unit = sender // 2
        gives = (
            ((z == 0) & ((unit == 1) | (unit == 2)))
            | ((z == 1) & (unit == 2))
            | ((z == 2) & (unit == 3))
            | ((z == 3) & (unit < 2))
        )

        @pl.when(gives)
        def _():
            came_back(sender)
            cols_ref[dev] += returned_ref[sender]

    loop(8, collect)
    row_back(1, beside).wait_recv()
    row_back(2, opposite).wait_recv()
    total = cols_ref[dev] + rows_in[0] + rows_in[1]
    out_ref[...] = jnp.log(total / counts_ref[...])

    pairing.wait_send()
    joining.wait_send()
    whole_sent(z, core_sems)
    remote(queries.at[:, 0], queries.at[:, 1], flow_sems.at[0], side_sems.at[0], beside).wait_send()
    remote(queries.at[:, 1], queries.at[:, 2], flow_sems.at[1], relay_sems.at[0], across).wait_send()
    row_back(1, beside).wait_send()
    row_back(2, opposite).wait_send()
    for n in range(7):
        scale_out(n).wait_send()

    def scale_rest(at):
        unit = at // 2
        used = (
            (unit == z)
            | ((z == 0) & (unit == 3))
            | ((z == 1) & ((unit == 0) | (unit == 3)))
            | ((z == 2) & (unit < 2))
            | ((z == 3) & (unit == 2))
        )

        @pl.when(jnp.logical_not(used))
        def _():
            remote(
                kscale_ref.at[at], kscale_ref.at[at],
                scale_sems.at[0, 0], scale_sems.at[1, at], partner,
            ).wait_recv()

    loop(8, scale_rest)

    def returns_sent(unit):
        loop(2, lambda c: give_back(2 * unit + c).wait_send())

    whole_sent(z, z_sems)

    @pl.when((z == 0) | (z == 3))
    def _():
        lower.wait_send()

    @pl.when((z == 1) | (z == 2))
    def _():
        rising.wait_send()
        outward_up.wait_send()

    @pl.when(z == 0)
    def _():
        whole_sent(3, core_sems)
        returns_sent(3)

    @pl.when(z == 1)
    def _():
        whole_sent(0, z_sems)
        whole_sent(3, z_sems)
        whole_sent(0, core_sems)
        whole_sent(3, core_sems)
        returns_sent(0)
        returns_sent(3)

    @pl.when(z == 2)
    def _():
        whole_sent(3, z_sems)
        for unit in (0, 1):
            whole_sent(unit, core_sems)
            returns_sent(unit)

    @pl.when(z == 3)
    def _():
        whole_sent(2, core_sems)
        returns_sent(2)


def gathered(documents, cluster_of, neighbours, sharpness):
    rows, width = documents.shape
    span = width // PIECES
    half = PIECES // 2
    vmem = pl.BlockSpec(memory_space=pltpu.VMEM)
    smem = pl.BlockSpec(memory_space=pltpu.SMEM)
    f32 = functools.partial(pltpu.VMEM, dtype=jnp.float32)
    bf16 = functools.partial(pltpu.VMEM, dtype=jnp.bfloat16)
    sems = pltpu.SemaphoreType.DMA
    density = pl.pallas_call(
        density_kernel,
        out_shape=jax.ShapeDtypeStruct((1, rows), jnp.float32),
        in_specs=[pl.BlockSpec(memory_space=pl.ANY), vmem, smem, smem],
        out_specs=vmem,
        scratch_shapes=[
            bf16((8, PIECES, rows, span)),
            bf16((PIECES, 3, rows, span)),
            f32((PIECES, 8, span)),
            f32((half, 8, span)),
            f32((half, 8, span)),
            f32((half, 8, span)),
            f32((half, 8, span)),
            f32((half, 8, span)),
            f32((PIECES, 8, span)),
            bf16((PIECES, 24, span)),
            f32((PIECES, rows, span)),
            f32((rows, span)),
            pltpu.VMEM((10, 1, rows), jnp.int32),
            f32((3, 3, rows, 1)),
            f32((3, rows, 1)),
            f32((8, 3, 1, rows)),
            f32((8, 1, rows)),
            f32((8, 1, rows)),
            f32((1, rows)),
            f32((3 * rows, 24)),
            bf16((3 * rows, 72)),
            f32((8, 3 * rows, rows)),
            f32((3, rows, rows)),
            f32((8, 1, rows)),
            f32((8, 1, rows)),
            f32((3, 1, rows)),
            f32((2, 1, rows)),
            sems((PIECES,)),
            sems((5, 2)),
            sems((4,)),
            sems((4,)),
            sems((8, PIECES)),
            sems((PIECES,)),
            sems((PIECES,)),
            sems((2,)),
            sems((2, 8)),
            sems((2, 8)),
            sems((2, 2)),
        ],
        compiler_params=pltpu.CompilerParams(
            collective_id=0, has_side_effects=True, vmem_limit_bytes=56 * 1024 * 1024
        ),
        name="density",
    )(documents, cluster_of.reshape(-1, 128), neighbours.T, sharpness)
    return density.reshape(rows)


def solution(mesh):
    small = mesh.shape["dev"] == 8 and mesh.shape["outer"] == 4
    in_specs = (P(("outer", "dev"), None), P(), P(), P())
    out_specs = P(("outer", "dev"))
    body = gathered if small else shards
    return jax.shard_map(body, mesh=mesh, in_specs=in_specs, out_specs=out_specs, check_vma=False)
```
